32 devices in a mesh: row: 4 (over x, core), col: 8 (over z, y).
Axes of the slice: x: 2, y: 2, z: 4, core: 2. Of those that a mesh axis runs over, the one named last changes fastest.
Arguments:
- tail_vectors: float32 [16128, 4096], P('row', 'col'), may hold values from -6 to 6
- lower_panel: float32 [16128, 1024], P(('row', 'col')), may hold values from -0.046875 to 0.046875
- window_rhs: float32 [1024, 4096], P('row', 'col'), may hold values from -6 to 6
- window_block: float32 [1024, 1024], P(('row', 'col')), may hold values from -1 to 2, as said below
Outputs:
- window_vectors: float32 [1024, 4096], P('row', 'col')
The draws below stay inside these ranges and needn't reach their ends.
Inputs may be any that keep to these rules, and one draw needn't show every extreme that they name: window_block is zero above the diagonal; its diagonal lies in 1 to 2; entries below the diagonal are under 1 / sqrt(1024) in magnitude.
All inputs are finite; a program needn't handle non-finite values.
Results may differ from the reference program's by a relative error of at most 0.000082.
Values sent between devices are 32-bit elements; how exact they have to be, the bound alone decides.
A program may use at most 128 MiB of HBM per device.

```python
import jax
import jax.numpy as jnp
from jax import lax

NEV = 4096
WIN = 1024
TAIL = 16128


def draw_window_block(key, part):
    key_lower = jax.random.fold_in(key, 11)
    key_diag = jax.random.fold_in(key, 12)
    lower_mask = jnp.tril(jnp.ones((WIN, WIN), jnp.float32), -1)
    magnitude = 1.0 / jnp.sqrt(jnp.float32(WIN))
    spread = 0.98 * jax.random.uniform(key_lower, (WIN, WIN), jnp.float32, -1.0, 1.0)
    diagonal = jnp.exp(jax.random.uniform(key_diag, (WIN,), jnp.float32, 0.0, 0.69))
    return lower_mask * spread * magnitude + jnp.diag(diagonal)


def shard_levels(key, dims, cuts, smallest, high):
    factor_of, own = 1.0, jax.random.fold_in(key, 6)
    for position, parts in cuts:
        steps = jnp.exp(jax.random.uniform(jax.random.fold_in(own, position), (parts,), jnp.float32, smallest / len(cuts), high / len(cuts)))
        factor_of = factor_of * jnp.repeat(steps, dims[position] // parts).reshape([-1 if axis == position else 1 for axis in range(len(dims))])
    return factor_of


def centred(own_key, extent, scale, limit, shards=(), kind=jnp.bfloat16):
    drawn = jax.random.normal(own_key, extent, jnp.float32) * scale
    if len(shards) > 0:
        drawn = shard_levels(own_key, extent, shards, -0.22, 0.18) * drawn
    return jnp.clip(drawn, min=-limit, max=limit).astype(kind)


def setup_inputs(seed: int = 0) -> dict:
    key_list = jax.random.split(jax.random.key(seed), 5)
    return {
        "tail_vectors": centred(key_list[0], (TAIL, NEV), 1.0, 6.0, ((0, 4), (1, 8)), jnp.float32),
        "lower_panel": centred(key_list[1], (TAIL, WIN), TAIL ** -0.5, 0.046875, ((0, 32),), jnp.float32),
        "window_rhs": centred(key_list[2], (WIN, NEV), 1.0, 6.0, ((0, 4), (1, 8)), jnp.float32),
        "window_block": draw_window_block(jax.random.fold_in(key_list[4], 71), 0),
    }


def reference(tail_vectors, lower_panel, window_rhs, window_block):
    correction = lax.dot_general(lower_panel.astype(jnp.float32), tail_vectors.astype(jnp.float32), (((0,), (0,)), ((), ())), precision=lax.Precision.HIGHEST, preferred_element_type=jnp.float32)
    right_side = window_rhs - correction
    return jax.scipy.linalg.solve_triangular(window_block, right_side, trans=1, lower=True)
```

```python
import functools

import jax
import jax.numpy as jnp
from jax import lax
from jax.experimental import pallas as pl
from jax.experimental.pallas import tpu as pltpu
from jax.sharding import PartitionSpec as P

MESH = pl.DeviceIdType.MESH
HIGHEST = lax.Precision.HIGHEST


def ring_sides(n):
    y = 1
    while (2 * y) * (2 * y) <= n:
        y *= 2
    return n // y, y


def col_of_position(pos, n):
    zs, ys = ring_sides(n)
    rest = jnp.maximum(pos - zs, 0)
    row = rest // (ys - 1)
    within = rest % (ys - 1)
    y = jnp.where(row % 2 == 0, 1 + within, ys - 1 - within)
    return jnp.where(pos < zs, pos * ys, (zs - 1 - row) * ys + y)


def position_of_col(col, n):
    zs, ys = ring_sides(n)
    z, y = col // ys, col % ys
    row = zs - 1 - z
    within = jnp.where(row % 2 == 0, y - 1, ys - 1 - y)
    return jnp.where(y == 0, z, zs + row * (ys - 1) + within)


def dot(a, b):
    return jnp.dot(a, b, precision=HIGHEST, preferred_element_type=jnp.float32)


def dot_t(a, b):
    return lax.dot_general(
        a, b, (((0,), (0,)), ((), ())), precision=HIGHEST, preferred_element_type=jnp.float32
    )


def lower_inverse(block, base=32):
    size = block.shape[0]
    rows = lax.broadcasted_iota(jnp.int32, (size, size), 0)
    cols = lax.broadcasted_iota(jnp.int32, (size, size), 1)
    eye = jnp.where(rows == cols, 1.0, 0.0)
    diag_col = jnp.sum(jnp.where(rows == cols, block, 0.0), axis=1, keepdims=True)
    diag_row = jnp.sum(jnp.where(rows == cols, block, 0.0), axis=0, keepdims=True)
    near = (rows // base == cols // base) & (rows > cols)
    power = jnp.where(near, -block / diag_col, 0.0)
    inverse = eye + power
    reach = 2
    while reach < base:
        power = dot(power, power)
        inverse = inverse + dot(inverse, power)
        reach *= 2
    inverse = inverse / diag_row
    while base < size:
        below = (rows // (2 * base) == cols // (2 * base)) & (rows // base > cols // base)
        inverse = inverse - dot(dot(inverse, jnp.where(below, block, 0.0)), inverse)
        base *= 2
    return inverse


def kernel(
    n, groups, tail_hbm, panel_hbm, block_hbm, rhs_ref, out_ref,
    tail, buf, acc, strip, inverse, solved, parts, landed,
    tail_sem, load_sem, send_sem, recv_sem, part_send, part_recv,
):
    half = n // 2
    depth = panel_hbm.shape[0]
    thin = block_hbm.shape[0]
    width = buf.shape[-1]
    r = lax.axis_index("row")
    me = position_of_col(lax.axis_index("col"), n)
    right = col_of_position((me + 1) % n, n)
    left = col_of_position((me + n - 1) % n, n)

    tail_copy = pltpu.make_async_copy(tail_hbm, tail, tail_sem)

    def loads(g):
        cols = pl.ds(pl.multiple_of((groups - 1 - g) * width, width), width)
        return (
            pltpu.make_async_copy(panel_hbm.at[:, cols], buf.at[0, g, pl.ds(0, depth)], load_sem.at[0, g]),
            pltpu.make_async_copy(block_hbm.at[:, cols], buf.at[0, g, pl.ds(depth, thin)], load_sem.at[1, g]),
        )

    def start_loads(g, _):
        for copy in loads(g):
            copy.start()
        return 0

    lax.fori_loop(0, groups, start_loads, 0)
    tail_copy.start()

    barrier = pltpu.get_barrier_semaphore()
    for side in (left, right):
        pl.semaphore_signal(barrier, inc=1, device_id={"col": side}, device_id_type=MESH)
    for k in range(1, groups):
        pl.semaphore_signal(barrier, inc=1, device_id={"row": (r + k) % groups}, device_id_type=MESH)
    pl.semaphore_wait(barrier, 2 + groups - 1)

    def hop(way, g, d):
        source = d - 1 if way == 0 else (n - (d - 1)) % n
        target = d if way == 0 else n - d
        return pltpu.make_async_remote_copy(
            src_ref=buf.at[source, g],
            dst_ref=buf.at[target, g],
            send_sem=send_sem.at[way, g, d - 1],
            recv_sem=recv_sem.at[way, g, d - 1],
            device_id={"col": right if way == 0 else left},
            device_id_type=MESH,
        )

    def send_own(g):
        for copy in loads(g):
            copy.wait()
        for way in range(2):
            hop(way, g, 1).start()

    def use(slot, g):
        origin = col_of_position((me + n - slot) % n, n)
        rows = pl.ds(pl.multiple_of(origin * depth, 8), depth)
        acc[...] += dot_t(buf[slot, g, pl.ds(0, depth)], tail[rows, :])
        strip[pl.ds(pl.multiple_of(origin * thin, 8), thin), :] = buf[slot, g, pl.ds(depth, thin)]

    def part_copy(q):
        return pltpu.make_async_remote_copy(
            src_ref=parts.at[q],
            dst_ref=landed.at[r],
            send_sem=part_send.at[q],
            recv_sem=part_recv.at[r],
            device_id={"row": q},
            device_id_type=MESH,
        )

    def finish(q):
        total = parts[q]
        for k in range(1, groups):
            other = (r + k) % groups
            pltpu.make_async_remote_copy(
                src_ref=parts.at[q],
                dst_ref=landed.at[other],
                send_sem=part_send.at[q],
                recv_sem=part_recv.at[other],
                device_id={"row": other},
                device_id_type=MESH,
            ).wait_recv()
            total = total + landed[other]
        solved[...] = dot_t(inverse[...], total)
        out_ref[...] = solved[...]

    send_own(0)
    tail_copy.wait()

    def group(g, _):
        q = groups - 1 - g

        @pl.when(g + 1 < groups)
        def _():
            send_own(g + 1)

        acc[...] = jnp.zeros_like(acc)
        use(0, g)

        def step(d, _):
            for way in range(2):
                hop(way, g, d).wait_recv()
                onward = d + 1 < half
                last = (d + 1 == half) & (g % 2 == way)

                @pl.when(onward | last)
                def _():
                    hop(way, g, d + 1).start()

            def both(way, _):
                use(jnp.where(way == 0, d, n - d), g)
                return 0

            lax.fori_loop(0, 2, both, 0)

            @pl.when((d == half - 1) & (r == q + 1))
            def _():
                finish(q + 1)

            return 0

        lax.fori_loop(1, half, step, 0)
        for way in range(2):
            @pl.when(g % 2 == way)
            def _():
                hop(way, g, half).wait_recv()

        use(half, g)

        parts[q] = -acc[...]

        @pl.when(r == q)
        def _():
            parts[q] += rhs_ref[...]

        @pl.when(r > q)
        def _():
            parts[q] -= dot_t(strip[...], solved[...])

        @pl.when(r != q)
        def _():
            part_copy(q).start()

        @pl.when(r == q)
        def _():
            inverse[...] = lower_inverse(strip[...])

        return 0

    lax.fori_loop(0, groups, group, 0)

    @pl.when(r == 0)
    def _():
        finish(0)

    def drain(g, _):
        def one(d, _):
            for way in range(2):
                @pl.when((d < half) | (g % 2 == way))
                def _():
                    hop(way, g, d).wait_send()
            return 0

        lax.fori_loop(1, half + 1, one, 0)

        @pl.when(r != g)
        def _():
            part_copy(g).wait_send()

        return 0

    lax.fori_loop(0, groups, drain, 0)


def per_device(n, groups, tail_vectors, lower_panel, window_rhs, window_block):
    tail_rows, columns = tail_vectors.shape
    depth, window = lower_panel.shape
    thin = window_block.shape[0]
    width = window // groups
    half = n // 2
    f32 = jnp.float32
    anywhere = pl.BlockSpec(memory_space=pl.ANY)
    vmem = pl.BlockSpec(memory_space=pltpu.VMEM)
    return pl.pallas_call(
        functools.partial(kernel, n, groups),
        out_shape=jax.ShapeDtypeStruct((width, columns), f32),
        in_specs=[anywhere, anywhere, anywhere, vmem],
        out_specs=vmem,
        scratch_shapes=[
            pltpu.VMEM((tail_rows, columns), f32),
            pltpu.VMEM((n, groups, depth + thin, width), f32),
            pltpu.VMEM((width, columns), f32),
            pltpu.VMEM((width, width), f32),
            pltpu.VMEM((width, width), f32),
            pltpu.VMEM((width, columns), f32),
            pltpu.VMEM((groups, width, columns), f32),
            pltpu.VMEM((groups, width, columns), f32),
            pltpu.SemaphoreType.DMA,
            pltpu.SemaphoreType.DMA((2, groups)),
            pltpu.SemaphoreType.DMA((2, groups, half)),
            pltpu.SemaphoreType.DMA((2, groups, half)),
            pltpu.SemaphoreType.DMA((groups,)),
            pltpu.SemaphoreType.DMA((groups,)),
        ],
        compiler_params=pltpu.CompilerParams(
            collective_id=0, has_side_effects=True, vmem_limit_bytes=60 * 1024 * 1024
        ),
    )(tail_vectors, lower_panel, window_block, window_rhs)


def solution(mesh):
    in_specs = (P("row", "col"), P(("row", "col"), None), P("row", "col"), P(("row", "col"), None))
    out_specs = P("row", "col")
    body = functools.partial(per_device, mesh.shape["col"], mesh.shape["row"])
    return jax.shard_map(body, mesh=mesh, in_specs=in_specs, out_specs=out_specs, check_vma=False)
```

```python
import functools

import jax
import jax.numpy as jnp
from jax import lax
from jax.experimental import pallas as pl
from jax.experimental.pallas import tpu as pltpu
from jax.sharding import PartitionSpec as P

MESH = pl.DeviceIdType.MESH
HIGHEST = lax.Precision.HIGHEST


def ring_sides(n):
    y = 1
    while (2 * y) * (2 * y) <= n:
        y *= 2
    return n // y, y


def col_of_position(pos, n):
    zs, ys = ring_sides(n)
    rest = jnp.maximum(pos - zs, 0)
    row = rest // (ys - 1)
    within = rest % (ys - 1)
    y = jnp.where(row % 2 == 0, 1 + within, ys - 1 - within)
    return jnp.where(pos < zs, pos * ys, (zs - 1 - row) * ys + y)


def position_of_col(col, n):
    zs, ys = ring_sides(n)
    z, y = col // ys, col % ys
    row = zs - 1 - z
    within = jnp.where(row % 2 == 0, y - 1, ys - 1 - y)
    return jnp.where(y == 0, z, zs + row * (ys - 1) + within)


def dot(a, b):
    return jnp.dot(a, b, precision=HIGHEST, preferred_element_type=jnp.float32)


def dot_t(a, b):
    return lax.dot_general(
        a, b, (((0,), (0,)), ((), ())), precision=HIGHEST, preferred_element_type=jnp.float32
    )


def lower_inverse(block, base=32):
    size = block.shape[0]
    rows = lax.broadcasted_iota(jnp.int32, (size, size), 0)
    cols = lax.broadcasted_iota(jnp.int32, (size, size), 1)
    eye = jnp.where(rows == cols, 1.0, 0.0)
    diag_col = jnp.sum(jnp.where(rows == cols, block, 0.0), axis=1, keepdims=True)
    diag_row = jnp.sum(jnp.where(rows == cols, block, 0.0), axis=0, keepdims=True)
    near = (rows // base == cols // base) & (rows > cols)
    power = jnp.where(near, -block / diag_col, 0.0)
    inverse = eye + power
    reach = 2
    while reach < base:
        power = dot(power, power)
        inverse = inverse + dot(inverse, power)
        reach *= 2
    inverse = inverse / diag_row
    while base < size:
        below = (rows // (2 * base) == cols // (2 * base)) & (rows // base > cols // base)
        inverse = inverse - dot(dot(inverse, jnp.where(below, block, 0.0)), inverse)
        base *= 2
    return inverse


WIDTH = 128
STRIDE_D, STRIDE_G = 4, 3


def kernel(
    n, rows_axis, tail_hbm, panel_hbm, block_hbm, rhs_ref, out_ref,
    tail, buf, strips, inverse, solved, parts, landed,
    tail_sem, load_sem, send_sem, recv_sem, part_send, part_recv,
):
    half = n // 2
    depth = panel_hbm.shape[0]
    thin = block_hbm.shape[0]
    groups, width = buf.shape[1], buf.shape[-1]
    per_row = groups // rows_axis
    r = lax.axis_index("row")
    me = position_of_col(lax.axis_index("col"), n)
    right = col_of_position((me + 1) % n, n)
    left = col_of_position((me + n - 1) % n, n)

    def loads(g):
        cols = pl.ds(pl.multiple_of((groups - 1 - g) * width, width), width)
        return (
            pltpu.make_async_copy(panel_hbm.at[:, cols], buf.at[0, g, pl.ds(0, depth)], load_sem.at[0, g]),
            pltpu.make_async_copy(block_hbm.at[:, cols], buf.at[0, g, pl.ds(depth, thin)], load_sem.at[1, g]),
        )

    def start_loads(g, _):
        for copy in loads(g):
            copy.start()
        return 0

    lax.fori_loop(0, groups, start_loads, 0)
    tail_copy = pltpu.make_async_copy(tail_hbm, tail, tail_sem)
    tail_copy.start()

    barrier = pltpu.get_barrier_semaphore()
    for side in (left, right):
        pl.semaphore_signal(barrier, inc=1, device_id={"col": side}, device_id_type=MESH)
    for k in range(1, rows_axis):
        pl.semaphore_signal(barrier, inc=1, device_id={"row": (r + k) % rows_axis}, device_id_type=MESH)
    pl.semaphore_wait(barrier, 2 + rows_axis - 1)

    def hop(way, g, d):
        source = d - 1 if way == 0 else (n - (d - 1)) % n
        target = d if way == 0 else n - d
        return pltpu.make_async_remote_copy(
            src_ref=buf.at[source, g],
            dst_ref=buf.at[target, g],
            send_sem=send_sem.at[way, g, d - 1],
            recv_sem=recv_sem.at[way, g, d - 1],
            device_id={"col": right if way == 0 else left},
            device_id_type=MESH,
        )

    def use(slot, g):
        origin = col_of_position((me + n - slot) % n, n)
        rows = pl.ds(pl.multiple_of(origin * depth, 8), depth)
        parts[g] -= dot_t(buf[slot, g, pl.ds(0, depth)], tail[rows, :])
        strips[g, pl.ds(pl.multiple_of(origin * thin, 8), thin), :] = buf[slot, g, pl.ds(depth, thin)]

    def part_copy(g, source, owner):
        slot = (groups - 1 - g) % per_row
        return pltpu.make_async_remote_copy(
            src_ref=parts.at[g],
            dst_ref=landed.at[slot, source],
            send_sem=part_send.at[g],
            recv_sem=part_recv.at[slot, source],
            device_id={"row": owner},
            device_id_type=MESH,
        )

    def place(g):
        return pl.ds(pl.multiple_of(((groups - 1 - g) % per_row) * width, width), width)

    def owner_of(g):
        return (groups - 1 - g) // per_row

    def finish(g):
        total = parts[g]
        for k in range(1, rows_axis):
            other = (r + k) % rows_axis
            part_copy(g, other, other).wait_recv()
            total = total + landed[(groups - 1 - g) % per_row, other]
        result = dot_t(inverse[...], total)
        solved[place(g), :] = result
        out_ref[place(g), :] = result

    def clear(g, _):
        parts[g] = jnp.zeros_like(parts[g])

        @pl.when(r == owner_of(g))
        def _():
            parts[g] = rhs_ref[place(g), :]

        return 0

    lax.fori_loop(0, groups, clear, 0)
    solved[...] = jnp.zeros_like(solved)

    def complete(g):
        @pl.when((g > 0) & (r == owner_of(g - 1)))
        def _():
            finish(g - 1)

        @pl.when(r >= owner_of(g))
        def _():
            parts[g] -= dot_t(strips[g], solved[...])

        @pl.when(r != owner_of(g))
        def _():
            part_copy(g, r, owner_of(g)).start()

        @pl.when(r == owner_of(g))
        def _():
            inverse[...] = lower_inverse(strips[g, place(g), :])

    def item(g, d):
        @pl.when(d == 0)
        def _():
            for copy in loads(g):
                copy.wait()
            for way in range(2):
                hop(way, g, 1).start()

        @pl.when((d == 0) & (g == 0))
        def _():
            tail_copy.wait()

        for way in range(2):
            @pl.when((d > 0) & ((d < half) | (g % 2 == way)))
            def _():
                hop(way, g, d).wait_recv()

            @pl.when((d > 0) & ((d + 1 < half) | ((d + 1 == half) & (g % 2 == way))))
            def _():
                hop(way, g, d + 1).start()

        def one(way, _):
            use(jnp.where(way == 0, d, n - d), g)
            return 0

        lax.fori_loop(0, jnp.where((d == 0) | (d == half), 1, 2), one, 0)

        @pl.when(d == half)
        def _():
            complete(g)

    def diagonal(k, _):
        def one(g, _):
            rest = k - STRIDE_G * g

            @pl.when((rest >= 0) & (rest <= STRIDE_D * half) & (rest % STRIDE_D == 0))
            def _():
                item(g, rest // STRIDE_D)

            return 0

        lax.fori_loop(0, groups, one, 0)
        return 0

    lax.fori_loop(0, STRIDE_D * half + STRIDE_G * (groups - 1) + 1, diagonal, 0)

    @pl.when(r == 0)
    def _():
        finish(groups - 1)

    def drain(g, _):
        def one(d, _):
            for way in range(2):
                @pl.when((d < half) | (g % 2 == way))
                def _():
                    hop(way, g, d).wait_send()
            return 0

        lax.fori_loop(1, half + 1, one, 0)

        @pl.when(r != owner_of(g))
        def _():
            part_copy(g, r, owner_of(g)).wait_send()

        return 0

    lax.fori_loop(0, groups, drain, 0)


def per_device(n, rows_axis, tail_vectors, lower_panel, window_rhs, window_block):
    tail_rows, columns = tail_vectors.shape
    depth, window = lower_panel.shape
    thin = window_block.shape[0]
    share = window // rows_axis
    width = min(WIDTH, share)
    groups = window // width
    half = n // 2
    f32 = jnp.float32
    anywhere = pl.BlockSpec(memory_space=pl.ANY)
    vmem = pl.BlockSpec(memory_space=pltpu.VMEM)
    return pl.pallas_call(
        functools.partial(kernel, n, rows_axis),
        out_shape=jax.ShapeDtypeStruct((share, columns), f32),
        in_specs=[anywhere, anywhere, anywhere, vmem],
        out_specs=vmem,
        scratch_shapes=[
            pltpu.VMEM((tail_rows, columns), f32),
            pltpu.VMEM((n, groups, depth + thin, width), f32),
            pltpu.VMEM((groups, share, width), f32),
            pltpu.VMEM((width, width), f32),
            pltpu.VMEM((share, columns), f32),
            pltpu.VMEM((groups, width, columns), f32),
            pltpu.VMEM((share // width, rows_axis, width, columns), f32),
            pltpu.SemaphoreType.DMA,
            pltpu.SemaphoreType.DMA((2, groups)),
            pltpu.SemaphoreType.DMA((2, groups, half)),
            pltpu.SemaphoreType.DMA((2, groups, half)),
            pltpu.SemaphoreType.DMA((groups,)),
            pltpu.SemaphoreType.DMA((share // width, rows_axis)),
        ],
        compiler_params=pltpu.CompilerParams(
            collective_id=0, has_side_effects=True, vmem_limit_bytes=60 * 1024 * 1024
        ),
    )(tail_vectors, lower_panel, window_block, window_rhs)


def solution(mesh):
    in_specs = (P("row", "col"), P(("row", "col"), None), P("row", "col"), P(("row", "col"), None))
    out_specs = P("row", "col")
    body = functools.partial(per_device, mesh.shape["col"], mesh.shape["row"])
    return jax.shard_map(body, mesh=mesh, in_specs=in_specs, out_specs=out_specs, check_vma=False)
```

```python
import functools

import jax
import jax.numpy as jnp
from jax import lax
from jax.experimental import pallas as pl
from jax.experimental.pallas import tpu as pltpu
from jax.sharding import PartitionSpec as P

MESH = pl.DeviceIdType.MESH
HIGHEST = lax.Precision.HIGHEST


def ring_sides(n):
    y = 1
    while (2 * y) * (2 * y) <= n:
        y *= 2
    return n // y, y


def col_of_position(pos, n):
    zs, ys = ring_sides(n)
    rest = jnp.maximum(pos - zs, 0)
    row = rest // (ys - 1)
    within = rest % (ys - 1)
    y = jnp.where(row % 2 == 0, 1 + within, ys - 1 - within)
    return jnp.where(pos < zs, pos * ys, (zs - 1 - row) * ys + y)


def position_of_col(col, n):
    zs, ys = ring_sides(n)
    z, y = col // ys, col % ys
    row = zs - 1 - z
    within = jnp.where(row % 2 == 0, y - 1, ys - 1 - y)
    return jnp.where(y == 0, z, zs + row * (ys - 1) + within)


def dot(a, b):
    return jnp.dot(a, b, precision=HIGHEST, preferred_element_type=jnp.float32)


def dot_t(a, b):
    return lax.dot_general(
        a, b, (((0,), (0,)), ((), ())), precision=HIGHEST, preferred_element_type=jnp.float32
    )


def lower_inverse(block, base=32):
    size = block.shape[0]
    rows = lax.broadcasted_iota(jnp.int32, (size, size), 0)
    cols = lax.broadcasted_iota(jnp.int32, (size, size), 1)
    eye = jnp.where(rows == cols, 1.0, 0.0)
    diag_col = jnp.sum(jnp.where(rows == cols, block, 0.0), axis=1, keepdims=True)
    diag_row = jnp.sum(jnp.where(rows == cols, block, 0.0), axis=0, keepdims=True)
    near = (rows // base == cols // base) & (rows > cols)
    power = jnp.where(near, -block / diag_col, 0.0)
    inverse = eye + power
    reach = 2
    while reach < base:
        power = dot(power, power)
        inverse = inverse + dot(inverse, power)
        reach *= 2
    inverse = inverse / diag_row
    while base < size:
        below = (rows // (2 * base) == cols // (2 * base)) & (rows // base > cols // base)
        inverse = inverse - dot(dot(inverse, jnp.where(below, block, 0.0)), inverse)
        base *= 2
    return inverse


WIDTH = 128
STRIDE_D, STRIDE_G = 4, 3


def kernel(
    n, rows_axis, tail_hbm, panel_hbm, block_hbm, rhs_hbm, out_ref,
    tail, rhs, buf, strips, inverse, solved, parts, landed,
    tail_sem, rhs_sem, load_sem, send_sem, recv_sem, part_send, part_recv,
):
    half = n // 2
    depth = panel_hbm.shape[0]
    thin = block_hbm.shape[0]
    groups, width = buf.shape[1], buf.shape[-1]
    per_row = groups // rows_axis
    r = lax.axis_index("row")
    me = position_of_col(lax.axis_index("col"), n)
    right = col_of_position((me + 1) % n, n)
    left = col_of_position((me + n - 1) % n, n)

    def loads(g):
        cols = pl.ds(pl.multiple_of((groups - 1 - g) * width, width), width)
        return (
            pltpu.make_async_copy(panel_hbm.at[:, cols], buf.at[0, g, pl.ds(0, depth)], load_sem.at[0, g]),
            pltpu.make_async_copy(block_hbm.at[:, cols], buf.at[0, g, pl.ds(depth, thin)], load_sem.at[1, g]),
        )

    def start_loads(g, _):
        for copy in loads(g):
            copy.start()
        return 0

    lax.fori_loop(0, groups, start_loads, 0)
    tail_copy = pltpu.make_async_copy(tail_hbm, tail, tail_sem)
    rhs_copy = pltpu.make_async_copy(rhs_hbm, rhs, rhs_sem)
    rhs_copy.start()
    tail_copy.start()

    barrier = pltpu.get_barrier_semaphore()
    for side in (left, right):
        pl.semaphore_signal(barrier, inc=1, device_id={"col": side}, device_id_type=MESH)
    for k in range(1, rows_axis):
        pl.semaphore_signal(barrier, inc=1, device_id={"row": (r + k) % rows_axis}, device_id_type=MESH)
    pl.semaphore_wait(barrier, 2 + rows_axis - 1)

    def hop(way, g, d):
        source = d - 1 if way == 0 else (n - (d - 1)) % n
        target = d if way == 0 else n - d
        return pltpu.make_async_remote_copy(
            src_ref=buf.at[source, g],
            dst_ref=buf.at[target, g],
            send_sem=send_sem.at[way, g, d - 1],
            recv_sem=recv_sem.at[way, g, d - 1],
            device_id={"col": right if way == 0 else left},
            device_id_type=MESH,
        )

    def use(slot, g):
        origin = col_of_position((me + n - slot) % n, n)
        rows = pl.ds(pl.multiple_of(origin * depth, 8), depth)
        parts[g] -= dot_t(buf[slot, g, pl.ds(0, depth)], tail[rows, :])
        strips[g, pl.ds(pl.multiple_of(origin * thin, 8), thin), :] = buf[slot, g, pl.ds(depth, thin)]

    def part_copy(g, source, owner):
        slot = (groups - 1 - g) % per_row
        return pltpu.make_async_remote_copy(
            src_ref=parts.at[g],
            dst_ref=landed.at[slot, source],
            send_sem=part_send.at[g],
            recv_sem=part_recv.at[slot, source],
            device_id={"row": owner},
            device_id_type=MESH,
        )

    def place(g):
        return pl.ds(pl.multiple_of(((groups - 1 - g) % per_row) * width, width), width)

    def owner_of(g):
        return (groups - 1 - g) // per_row

    def finish(g):
        total = parts[g]
        for k in range(1, rows_axis):
            other = (r + k) % rows_axis
            part_copy(g, other, other).wait_recv()
            total = total + landed[(groups - 1 - g) % per_row, other]
        result = dot_t(inverse[...], total)
        solved[place(g), :] = result
        out_ref[place(g), :] = result

    def clear(g, _):
        parts[g] = jnp.zeros_like(parts[g])

        @pl.when(r == owner_of(g))
        def _():
            parts[g] = rhs[place(g), :]

        return 0

    def complete(g):
        @pl.when((g > 0) & (r == owner_of(g - 1)))
        def _():
            finish(g - 1)

        @pl.when(r >= owner_of(g))
        def _():
            parts[g] -= dot_t(strips[g], solved[...])

        @pl.when(r != owner_of(g))
        def _():
            part_copy(g, r, owner_of(g)).start()

        @pl.when(r == owner_of(g))
        def _():
            inverse[...] = lower_inverse(strips[g, place(g), :])

    def item(g, d):
        @pl.when(d == 0)
        def _():
            for copy in loads(g):
                copy.wait()
            for way in range(2):
                hop(way, g, 1).start()

        @pl.when((d == 0) & (g == 0))
        def _():
            rhs_copy.wait()
            lax.fori_loop(0, groups, clear, 0)
            solved[...] = jnp.zeros_like(solved)
            tail_copy.wait()

        for way in range(2):
            @pl.when((d > 0) & ((d < half) | (g % 2 == way)))
            def _():
                hop(way, g, d).wait_recv()

            @pl.when((d > 0) & ((d + 1 < half) | ((d + 1 == half) & (g % 2 == way))))
            def _():
                hop(way, g, d + 1).start()

        def one(way, _):
            use(jnp.where(way == 0, d, n - d), g)
            return 0

        lax.fori_loop(0, jnp.where((d == 0) | (d == half), 1, 2), one, 0)

        @pl.when(d == half)
        def _():
            complete(g)

    def diagonal(k, _):
        def one(g, _):
            rest = k - STRIDE_G * g

            @pl.when((rest >= 0) & (rest <= STRIDE_D * half) & (rest % STRIDE_D == 0))
            def _():
                item(g, rest // STRIDE_D)

            return 0

        lax.fori_loop(0, groups, one, 0)
        return 0

    lax.fori_loop(0, STRIDE_D * half + STRIDE_G * (groups - 1) + 1, diagonal, 0)

    @pl.when(r == 0)
    def _():
        finish(groups - 1)

    def drain(g, _):
        def one(d, _):
            for way in range(2):
                @pl.when((d < half) | (g % 2 == way))
                def _():
                    hop(way, g, d).wait_send()
            return 0

        lax.fori_loop(1, half + 1, one, 0)

        @pl.when(r != owner_of(g))
        def _():
            part_copy(g, r, owner_of(g)).wait_send()

        return 0

    lax.fori_loop(0, groups, drain, 0)


def per_device(n, rows_axis, tail_vectors, lower_panel, window_rhs, window_block):
    tail_rows, columns = tail_vectors.shape
    depth, window = lower_panel.shape
    thin = window_block.shape[0]
    share = window // rows_axis
    width = min(WIDTH, share)
    groups = window // width
    half = n // 2
    f32 = jnp.float32
    anywhere = pl.BlockSpec(memory_space=pl.ANY)
    vmem = pl.BlockSpec(memory_space=pltpu.VMEM)
    return pl.pallas_call(
        functools.partial(kernel, n, rows_axis),
        out_shape=jax.ShapeDtypeStruct((share, columns), f32),
        in_specs=[anywhere] * 4,
        out_specs=vmem,
        scratch_shapes=[
            pltpu.VMEM((tail_rows, columns), f32),
            pltpu.VMEM((share, columns), f32),
            pltpu.VMEM((n, groups, depth + thin, width), f32),
            pltpu.VMEM((groups, share, width), f32),
            pltpu.VMEM((width, width), f32),
            pltpu.VMEM((share, columns), f32),
            pltpu.VMEM((groups, width, columns), f32),
            pltpu.VMEM((share // width, rows_axis, width, columns), f32),
            pltpu.SemaphoreType.DMA,
            pltpu.SemaphoreType.DMA,
            pltpu.SemaphoreType.DMA((2, groups)),
            pltpu.SemaphoreType.DMA((2, groups, half)),
            pltpu.SemaphoreType.DMA((2, groups, half)),
            pltpu.SemaphoreType.DMA((groups,)),
            pltpu.SemaphoreType.DMA((share // width, rows_axis)),
        ],
        compiler_params=pltpu.CompilerParams(
            collective_id=0, has_side_effects=True, vmem_limit_bytes=60 * 1024 * 1024
        ),
    )(tail_vectors, lower_panel, window_block, window_rhs)


def solution(mesh):
    in_specs = (P("row", "col"), P(("row", "col"), None), P("row", "col"), P(("row", "col"), None))
    out_specs = P("row", "col")
    body = functools.partial(per_device, mesh.shape["col"], mesh.shape["row"])
    return jax.shard_map(body, mesh=mesh, in_specs=in_specs, out_specs=out_specs, check_vma=False)
```
